8 devices in a mesh: dp: 1 (over z), tp: 8 (over x, y, core).
Axes of the slice: x: 2, y: 2, z: 1, core: 2. Of those that a mesh axis runs over, the one named last changes fastest.
Arguments:
- x: bfloat16 [128, 7168], P('dp')
- w_gate: bfloat16 [7168, 18432], P(None, 'tp')
- w_up: bfloat16 [7168, 18432], P(None, 'tp')
- w_down: bfloat16 [18432, 7168], P('tp')
Outputs:
- output: bfloat16 [128, 7168], P('dp')
All inputs are finite; a program needn't handle non-finite values.
Results may differ from the reference program's by a relative error of at most 0.016.
Values are sent between devices in bfloat16 or wider.
A program may use at most 2 GiB of HBM per device.

```python
import jax
import jax.numpy as jnp

ROWS = 128
D = 7168
FF = 18432


def setup_inputs(seed: int = 0, part: int = 0) -> dict:
    kx, kg, ku, kd = jax.random.split(jax.random.key(seed), 4)
    drawn = {
        "x": jax.random.normal(jax.random.fold_in(kx, part), (ROWS, D), jnp.float32),
        "w_gate": jax.random.normal(kg, (D, FF), jnp.float32) * D**-0.5,
        "w_up": jax.random.normal(ku, (D, FF), jnp.float32) * D**-0.5,
        "w_down": jax.random.normal(kd, (FF, D), jnp.float32) * FF**-0.5,
    }
    return {k: v.astype(jnp.bfloat16) for k, v in drawn.items()}


def reference(x, w_gate, w_up, w_down):
    gate = jnp.dot(x, w_gate, preferred_element_type=jnp.float32)
    up = jnp.dot(x, w_up, preferred_element_type=jnp.float32)
    hidden = (jax.nn.silu(gate) * up).astype(jnp.bfloat16)
    return jnp.dot(hidden, w_down, preferred_element_type=jnp.float32).astype(jnp.bfloat16)
```

```python
import functools

import jax
import jax.numpy as jnp
from jax import lax
from jax.experimental import pallas as pl
from jax.experimental.pallas import tpu as pltpu
from jax.sharding import PartitionSpec as P

BF = 256
SL = 2
KS = 4
NC = 512
LAGS = (1, 4, 7, 10, 13, 15)


def kernel(x_hbm, wg, wu, wd, y, xv, gb, ub, db, h, t, out, sa, ra, sb, rb, sc, rc,
           xs, gs, us, ds, ys, s1, r1, s2, r2):
    rows, d = xv.shape
    ff = h.shape[1]
    nf, nch, kb, hc = ff // BF, d // NC, d // KS, NC // 2
    me = lax.axis_index("tp")
    core, yb, xb = me % 2, (me // 2) % 2, me // 4
    mate, ynb, xnb = me + 1 - 2 * core, me + 2 - 4 * yb, me + 4 - 8 * xb
    first, second = (xnb, ynb), (ynb, xnb)
    fb, sbit = (xb, yb), (yb, xb)

    barrier = pltpu.get_barrier_semaphore()
    for other in (mate, ynb, xnb):
        pl.semaphore_signal(barrier, inc=1, device_id={"tp": other}, device_id_type=pl.DeviceIdType.MESH)

    def block(f, k):
        s = lax.rem(f, SL)
        src = (pl.ds(k * kb, kb), pl.ds(pl.multiple_of(f * BF, BF), BF))
        dst = (s, pl.ds(k * kb, kb))
        return (pltpu.make_async_copy(wg.at[src], gb.at[dst], gs.at[s, k]),
                pltpu.make_async_copy(wu.at[src], ub.at[dst], us.at[s, k]))

    def down(j):
        return pltpu.make_async_copy(wd.at[:, pl.ds(pl.multiple_of(j * NC, NC), NC)], db.at[j], ds.at[j])

    xcopy = pltpu.make_async_copy(x_hbm, xv, xs)
    xcopy.start()
    for f in range(SL):
        for k in range(KS):
            for c in block(f, k):
                c.start()
    xcopy.wait()

    def hidden(f, carry):
        s = lax.rem(f, SL)
        g = jnp.zeros((rows, BF), jnp.float32)
        u = jnp.zeros((rows, BF), jnp.float32)
        for k in range(KS):
            for c in block(f, k):
                c.wait()
            xk = xv[:, k * kb:(k + 1) * kb]
            g += jnp.dot(xk, gb[s, pl.ds(k * kb, kb)], preferred_element_type=jnp.float32)
            u += jnp.dot(xk, ub[s, pl.ds(k * kb, kb)], preferred_element_type=jnp.float32)
        h[:, pl.ds(pl.multiple_of(f * BF, BF), BF)] = (jax.nn.silu(g) * u).astype(jnp.bfloat16)

        @pl.when(f + SL < nf)
        def _():
            for k in range(KS):
                for c in block(f + SL, k):
                    c.start()

        @pl.when(f + SL == nf)
        def _():
            for j in range(nch):
                down(j).start()

        return carry

    lax.fori_loop(0, nf, hidden, 0)
    pl.semaphore_wait(barrier, 3)

    def remote(src, dst, i, dev):
        return pltpu.make_async_remote_copy(src_ref=src, dst_ref=dst, send_sem=s2.at[i], recv_sem=r2.at[i],
                                            device_id={"tp": dev}, device_id_type=pl.DeviceIdType.MESH)

    def at(n):
        return pl.ds(pl.multiple_of(n, 16), 16)

    def at32(n):
        return pl.ds(pl.multiple_of(n, 32), 32)

    half = core * 64

    def pair(j):
        return pltpu.make_async_remote_copy(src_ref=sa.at[j], dst_ref=ra.at[j], send_sem=s1.at[j], recv_sem=r1.at[j],
                                            device_id={"tp": mate}, device_id_type=pl.DeviceIdType.MESH)

    def send_b(j, c):
        return remote(sb.at[j, c], rb.at[j, c], 8 * j + c, first[c])

    def send_c(j, c):
        return remote(sc.at[j, c], rc.at[j, c], 8 * j + 2 + c, second[c])

    def send_d(j, c):
        r = out.at[j, c, at(half + 32 * fb[c] + 16 * sbit[c])]
        return remote(r, r, 8 * j + 4 + c, second[c])

    def send_e(j, c):
        r = out.at[j, c, at32(half + 32 * fb[c])]
        return remote(r, r, 8 * j + 6 + c, first[c])

    def send_f(j):
        r = out.at[j, :, pl.ds(pl.multiple_of(half, 64), 64)]
        return pltpu.make_async_remote_copy(src_ref=r, dst_ref=r, send_sem=s1.at[nch + j], recv_sem=r1.at[nch + j],
                                            device_id={"tp": mate}, device_id_type=pl.DeviceIdType.MESH)

    def result(j, c):
        cols = pl.ds(pl.multiple_of(j * NC + c * hc, hc), hc)
        return pltpu.make_async_copy(out.at[j, c], y.at[:, cols], ys.at[j, c])

    def matmul(j):
        down(j).wait()
        p = jnp.dot(h[...], db[j], preferred_element_type=jnp.float32)
        for c in range(2):
            t[j, c] = p[:, c * hc:(c + 1) * hc]
        for c in range(2):
            sa[j, c] = t[j, c, pl.ds(pl.multiple_of(64 - half, 64), 64)].astype(jnp.bfloat16)
        pair(j).start()

    def after_a(j):
        pair(j).wait_recv()
        for c in range(2):
            o = 32 * (1 - fb[c])
            v = t[j, c, at32(half + o)] + ra[j, c, at32(o)].astype(jnp.float32)
            sb[j, c] = v.astype(jnp.bfloat16)
            send_b(j, c).start()

    def after_b(j):
        for c in range(2):
            send_b(j, c).wait_recv()
            o = 16 * (1 - sbit[c])
            w = 32 * fb[c] + o
            v = t[j, c, at(half + w)] + ra[j, c, at(w)].astype(jnp.float32)
            v += rb[j, c, at(o)].astype(jnp.float32)
            sc[j, c] = v.astype(jnp.bfloat16)
            send_c(j, c).start()

    def after_c(j):
        for c in range(2):
            send_c(j, c).wait_recv()
            o = 16 * sbit[c]
            w = 32 * fb[c] + o
            v = t[j, c, at(half + w)] + ra[j, c, at(w)].astype(jnp.float32)
            v += rb[j, c, at(o)].astype(jnp.float32)
            v += rc[j, c].astype(jnp.float32)
            out[j, c, at(half + w)] = v.astype(jnp.bfloat16)
            send_d(j, c).start()

    def after_d(j):
        for c in range(2):
            send_d(j, c).wait_recv()
            send_e(j, c).start()

    def after_e(j):
        for c in range(2):
            send_e(j, c).wait_recv()
        send_f(j).start()

    def after_f(j):
        send_f(j).wait_recv()
        for c in range(2):
            result(j, c).start()

    stages = (after_a, after_b, after_c, after_d, after_e, after_f)

    def turn(i, carry):
        @pl.when(i < nch)
        def _():
            matmul(i)

        for lag, stage in zip(LAGS, stages):
            @pl.when(jnp.logical_and(i >= lag, i < nch + lag))
            def _(lag=lag, stage=stage):
                stage(i - lag)

        return carry

    lax.fori_loop(0, nch + LAGS[-1], turn, 0)

    def drain(j, carry):
        pair(j).wait_send()
        for c in range(2):
            for send in (send_b, send_c, send_d, send_e):
                send(j, c).wait_send()
            result(j, c).wait()
        send_f(j).wait_send()
        return carry

    lax.fori_loop(0, nch, drain, 0)


def solution(mesh):
    def step(x, w_gate, w_up, w_down):
        rows, d = x.shape
        ff = w_gate.shape[1]
        nch, hc = d // NC, NC // 2
        bf16, dma = jnp.bfloat16, pltpu.SemaphoreType.DMA
        anywhere = pl.BlockSpec(memory_space=pl.ANY)
        return pl.pallas_call(
            kernel,
            out_shape=jax.ShapeDtypeStruct((rows, d), bf16),
            in_specs=[anywhere] * 4,
            out_specs=anywhere,
            scratch_shapes=[
                pltpu.VMEM((rows, d), bf16),
                pltpu.VMEM((SL, d, BF), bf16),
                pltpu.VMEM((SL, d, BF), bf16),
                pltpu.VMEM((nch, ff, NC), bf16),
                pltpu.VMEM((rows, ff), bf16),
                pltpu.VMEM((nch, 2, rows, hc), jnp.float32),
                pltpu.VMEM((nch, 2, rows, hc), bf16),
                pltpu.VMEM((nch, 2, rows // 2, hc), bf16),
                pltpu.VMEM((nch, 2, rows // 2, hc), bf16),
                pltpu.VMEM((nch, 2, rows // 4, hc), bf16),
                pltpu.VMEM((nch, 2, rows // 4, hc), bf16),
                pltpu.VMEM((nch, 2, rows // 8, hc), bf16),
                pltpu.VMEM((nch, 2, rows // 8, hc), bf16),
                dma,
                dma((SL, KS)),
                dma((SL, KS)),
                dma((nch,)),
                dma((nch, 2)),
                dma((2 * nch,)),
                dma((2 * nch,)),
                dma((8 * nch,)),
                dma((8 * nch,)),
            ],
            compiler_params=pltpu.CompilerParams(
                collective_id=0, has_side_effects=True, vmem_limit_bytes=67043328
            ),
        )(x, w_gate, w_up, w_down)

    return jax.shard_map(
        step,
        mesh=mesh,
        in_specs=(P("dp", None), P(None, "tp"), P(None, "tp"), P("tp", None)),
        out_specs=P("dp", None),
        check_vma=False,
    )
```
